256 devices in a mesh: zero: 8 (over z_hi, core), model: 32 (over z_lo, y, x).
Axes of the slice: x: 4, y: 4, z: 8 (z_hi: 4, z_lo: 2; z = z_hi * 2 + z_lo), core: 2. Of those that a mesh axis runs over, the one named last changes fastest.
Arguments:
- w_gate: float32 [5120, 13824], P('zero', 'model'), may hold values from -0.15625 to 0.15625
- first_gate: float32 [5120, 13824], P('zero', 'model'), may hold values from -0.078125 to 0.078125
- second_gate: float32 [5120, 13824], P('zero', 'model'), may hold values from -0.078125 to 0.078125
- w_up: float32 [5120, 13824], P('zero', 'model'), may hold values from -0.15625 to 0.15625
- first_up: float32 [5120, 13824], P('zero', 'model'), may hold values from -0.078125 to 0.078125
- second_up: float32 [5120, 13824], P('zero', 'model'), may hold values from -0.078125 to 0.078125
- norm_train: float32 [5120], P(('zero', 'model')), may hold values from 0.25 to 1.75
- norm_step: float32 [5120], P(('zero', 'model')), may hold values from -0.3 to 0.3
Outputs:
- ready_gate: bfloat16 [5120, 13824], P(None, 'model')
- ready_up: bfloat16 [5120, 13824], P(None, 'model')
- column_gate: float32 [13824], P('model')
- column_up: float32 [13824], P('model')
- serve_norm: bfloat16 [5120], replicated
- latest_gate: float32 [5120, 13824], P('zero', 'model')
- latest_up: float32 [5120, 13824], P('zero', 'model')
The draws below stay inside these ranges and needn't reach their ends.
All inputs are finite; a program needn't handle non-finite values. Where the reference program divides by a largest or mean magnitude, that divisor is 1e-20 or more.
Results may differ from the reference program's by a relative error of at most 0.001.
Values may be sent and summed in bfloat16 or wider, within the bound.
A program may use at most 128 MiB of HBM per device.

```python
import jax
import jax.numpy as jnp

D_MODEL = 5120
D_INNER = 13824


def strengthened(result, rng, source, target, parts, factor):
    def block_of(axis_at):
        return (jnp.arange(result.shape[axis_at]) // (result.shape[axis_at] // parts)).reshape((-1,) + (1,) * (result.ndim - 1 - axis_at))

    first = jax.random.permutation(rng, parts)[block_of(target)]
    second = (block_of(target) + parts // 2) % parts
    return jnp.where((block_of(source) == first) | (block_of(source) == second), factor * result, result)


def block_scale(stream_key, dims, split, smallest, largest):
    loudness, own = 1.0, jax.random.fold_in(stream_key, 6)
    for position, blocks in split:
        draws = jnp.exp(jax.random.uniform(jax.random.fold_in(own, position), (blocks,), jnp.float32, smallest / len(split), largest / len(split)))
        loudness = loudness * jnp.repeat(draws, dims[position] // blocks).reshape([-1 if axis == position else 1 for axis in range(len(dims))])
    return loudness


def scatter_about(stream_key, shape, spread, reach, pieces=(), dtype=jnp.bfloat16):
    loudness = block_scale(stream_key, shape, pieces, -0.22, 0.18) if pieces else 1.0
    values = jax.random.normal(stream_key, shape, jnp.float32) * spread * loudness
    return jnp.minimum(jnp.maximum(values, -reach), reach).astype(dtype)


def gaussian_with(key, shape, spread, most, split, heavy, kind=jnp.bfloat16):
    values = spread * jax.random.normal(key, shape, jnp.float32)
    if split:
        values = values * block_scale(key, shape, split, -0.22, 0.18)
    return jnp.clip(strengthened(values, jax.random.fold_in(key, 3), *heavy), -most, most).astype(kind)


def setup_inputs(seed: int = 0) -> dict:
    splits = jax.random.split(jax.random.key(seed), 9)
    w_gate = gaussian_with(splits[0], (D_MODEL, D_INNER), D_MODEL ** -0.5, 0.15625, ((0, 8), (1, 32)), (0, 1, 32, 2.75), jnp.float32)
    first_gate = scatter_about(splits[1], (D_MODEL, D_INNER), D_MODEL ** -0.5, 0.078125, ((0, 8), (1, 32)), jnp.float32)
    second_gate = scatter_about(splits[2], (D_MODEL, D_INNER), D_MODEL ** -0.5, 0.078125, ((0, 8), (1, 32)), jnp.float32)
    w_up = gaussian_with(splits[3], (D_MODEL, D_INNER), D_MODEL ** -0.5, 0.15625, ((0, 8), (1, 32)), (0, 1, 32, 2.75), jnp.float32)
    first_up = scatter_about(splits[4], (D_MODEL, D_INNER), D_MODEL ** -0.5, 0.078125, ((0, 8), (1, 32)), jnp.float32)
    second_up = scatter_about(splits[5], (D_MODEL, D_INNER), D_MODEL ** -0.5, 0.078125, ((0, 8), (1, 32)), jnp.float32)
    norm_train = jnp.clip(1.0 + 0.15 * jax.random.normal(splits[6], (D_MODEL,), jnp.float32), 0.25, 1.75)
    norm_step = jnp.clip(jax.random.uniform(splits[7], (D_MODEL,), jnp.float32, -0.3, 0.3) * block_scale(splits[7], (D_MODEL,), ((0, 256),), -0.4, 0.0), -0.3, 0.3)
    return dict(w_gate=w_gate, first_gate=first_gate, second_gate=second_gate, w_up=w_up, first_up=first_up, second_up=second_up, norm_train=norm_train, norm_step=norm_step)


learn_rate = 0.25
hold_rate = 0.8


def reference(w_gate, first_gate, second_gate, w_up, first_up, second_up, norm_train, norm_step):
    hold_gate = hold_rate * first_gate + second_gate
    latest_gate = w_gate - learn_rate * hold_gate
    hold_up = hold_rate * first_up + second_up
    latest_up = w_up - learn_rate * hold_up
    column_gate = jnp.max(jnp.abs(latest_gate), axis=0)
    ready_gate = (latest_gate / column_gate).astype(jnp.bfloat16)
    column_up = jnp.max(jnp.abs(latest_up), axis=0)
    ready_up = (latest_up / column_up).astype(jnp.bfloat16)
    serve_norm = (norm_train + norm_step).astype(jnp.bfloat16)
    return ready_gate, ready_up, column_gate, column_up, serve_norm, latest_gate, latest_up
```

```python
import functools

import jax
import jax.numpy as jnp
from jax import lax
from jax.experimental import pallas as pl
from jax.experimental.pallas import tpu as pltpu
from jax.sharding import PartitionSpec as P

learn_rate = 0.25
hold_rate = 0.8

LANES = 128
CHUNK = 48
AHEAD = 4
ZERO, MODEL, PLANE = 8, 32, 16

f32, bf16 = jnp.float32, jnp.bfloat16


def iota(shape, dim):
    return lax.broadcasted_iota(jnp.int32, shape, dim)


def kernel(
    wg, fg, sg, wu, fu, su, nt, ns,
    rg, ru, lg, lu, cols, norm,
    stage, nin, mx, n1, nz, n3, wide,
    in_sem, nin_sem, mx_send, mx_recv, n_send, n1_recv, nz_recv, n3_recv,
    send_sem, own_recv, fwd_recv, d2d_send, d2d_recv,
):
    zero, model = lax.axis_index("zero"), lax.axis_index("model")
    rows_n, wide_n = lg.shape
    pieces = rows_n // CHUNK
    gathered, latest = (rg, ru), (lg, lu)
    high = lax.div(zero, 2)

    def at_zero(z):
        return {"zero": lax.rem(z, ZERO), "model": model}

    right, left = lax.rem(zero + 2, ZERO), lax.rem(zero + 6, ZERO)
    far = lax.rem(zero + 4, ZERO)
    mate = zero + 1 - 2 * lax.rem(zero, 2)
    plane0 = lax.div(model, PLANE) * PLANE
    spot = model - plane0
    other_plane = lax.rem(model + PLANE, MODEL)

    barrier = pltpu.get_barrier_semaphore()
    for j in range(1, ZERO):
        pl.semaphore_signal(barrier, inc=1, device_id=at_zero(zero + j))
    for j in range(1, PLANE):
        pl.semaphore_signal(
            barrier, inc=1, device_id={"zero": zero, "model": plane0 + lax.rem(spot + j, PLANE)}
        )

    @pl.when(high >= 2)
    def _():
        pl.semaphore_signal(barrier, inc=1, device_id={"zero": zero, "model": other_plane})

    loads = {}
    for k in range(pieces):
        for a, group in enumerate(((wg, fg, sg), (wu, fu, su))):
            for i, ref in enumerate(group):
                rows = pl.ds(k * CHUNK, CHUNK)
                loads[a, k, i] = pltpu.make_async_copy(
                    ref.at[rows], stage.at[a * 3 + i, rows], in_sem.at[a * 3 + i, k]
                )
                loads[a, k, i].start()
    norm_loads = [
        pltpu.make_async_copy(ref, nin.at[pl.ds(i, 1)], nin_sem.at[i])
        for i, ref in enumerate((nt, ns))
    ]
    for c in norm_loads:
        c.start()

    best = [None] * 8
    for k in range(pieces):
        rows = slice(k * CHUNK, (k + 1) * CHUNK)
        for a in range(2):
            for i in range(3):
                loads[a, k, i].wait()
            w, first, second = (stage[a * 3 + i, rows, :] for i in range(3))
            hold = hold_rate * first + second
            new = w - learn_rate * hold
            latest[a][rows, :] = new
            top = jnp.max(jnp.abs(new), axis=1, keepdims=True)
            at = iota((CHUNK, LANES), 0) + k * CHUNK - iota((CHUNK, LANES), 1)
            for r in range(k * CHUNK // LANES, ((k + 1) * CHUNK - 1) // LANES + 1):
                line = jnp.max(jnp.where(at == r * LANES, top, 0.0), axis=0, keepdims=True)
                old = best[a * 4 + r]
                best[a * 4 + r] = line if old is None else jnp.maximum(old, line)
    for r in range(8):
        mx[zero, pl.ds(r, 1), :] = best[r]

    for c in norm_loads:
        c.wait()
    part = jnp.concatenate(
        [nin[0:1, :] + nin[1:2, :], jnp.zeros((1, LANES - nin.shape[1]), f32)], axis=1
    ).astype(bf16).astype(f32)
    width = nin.shape[1]
    begin = model * width
    lane0 = lax.rem(begin, LANES)
    turned = pltpu.roll(jnp.broadcast_to(part, (8, LANES)), lane0, 1)
    place = iota((8, LANES), 0) * LANES + iota((8, LANES), 1) - begin
    n1[spot] = jnp.where((place >= 0) & (place < width), turned, 0.0)

    @pl.when(high < 2)
    def _():
        pl.semaphore_wait(barrier, ZERO - 1 + PLANE - 1)

    @pl.when(high >= 2)
    def _():
        pl.semaphore_wait(barrier, ZERO - 1 + PLANE)

    def remote(src, dst, send, recv, to):
        return pltpu.make_async_remote_copy(
            src_ref=src, dst_ref=dst, send_sem=send, recv_sem=recv, device_id=to,
            device_id_type=pl.DeviceIdType.MESH,
        )

    def bytes_of(ref, sem):
        pltpu.make_async_copy(ref, ref, sem).wait()

    for j in (4, 5, 3, 6, 2, 7, 1):
        remote(mx.at[zero], mx.at[zero], mx_send, mx_recv, at_zero(zero + j)).start()
    for j in range(1, PLANE):
        to = {"zero": zero, "model": plane0 + lax.rem(spot + j, PLANE)}
        remote(n1.at[spot], n1.at[spot], n_send, n1_recv, to).start()

    bytes_of(mx.at[pl.ds(0, ZERO - 1)], mx_recv)
    bytes_of(mx.at[pl.ds(0, ZERO - 1)], mx_send)
    most = jnp.max(mx[...], axis=0)
    cols[...] = most

    def part_of(a, k, z):
        return gathered[a].at[pl.ds(k * CHUNK, CHUNK), pl.ds(pl.multiple_of(z * wide_n, LANES), wide_n)]

    def normalise(k):
        rows = slice(k * CHUNK, (k + 1) * CHUNK)
        at = iota((CHUNK, LANES), 0) + k * CHUNK - iota((CHUNK, LANES), 1)
        for a in range(2):
            top = None
            for r in range(k * CHUNK // LANES, ((k + 1) * CHUNK - 1) // LANES + 1):
                line = jnp.broadcast_to(most[a * 4 + r : a * 4 + r + 1], (CHUNK, LANES))
                part = jnp.max(jnp.where(at == r * LANES, line, 0.0), axis=1, keepdims=True)
                top = part if top is None else jnp.maximum(top, part)
            scaled = latest[a][rows, :] * (1.0 / top)
            gathered[a][rows, pl.ds(pl.multiple_of(zero * wide_n, LANES), wide_n)] = scaled.astype(bf16)

    def push(a, k, z):
        ref = part_of(a, k, z)
        remote(ref, ref, d2d_send, d2d_recv.at[a], at_zero(mate)).start()

    steps = [(0, k) for k in range(pieces)] + [(1, k) for k in range(pieces)]

    def send_own(i):
        a, k = steps[i]
        if i < pieces:
            normalise(k)
        for way, (b, to) in enumerate(((a, right), (1 - a, left))):
            ref = part_of(b, k, zero)
            remote(ref, ref, send_sem.at[way], own_recv.at[way, i], at_zero(to)).start()
        if i < pieces:
            push(0, k, zero)
            push(1, k, zero)

    def arrive(way, i):
        a, k = steps[i]
        b, origin = ((a, left), (1 - a, right))[way]
        ref = part_of(b, k, origin)
        remote(ref, ref, send_sem.at[way], own_recv.at[way, i], at_zero(origin)).wait_recv()
        if i < pieces:
            to = (right, left)[way]
            remote(ref, ref, send_sem.at[way], fwd_recv.at[way, k], at_zero(to)).start()
        push(b, k, origin)

    def arrive_far(way, k):
        ref = part_of(way, k, far)
        remote(ref, ref, send_sem.at[way], fwd_recv.at[way, k], at_zero(far)).wait_recv()
        push(way, k, far)

    for i in range(AHEAD):
        send_own(i)
    far_done = 0
    for i in range(2 * pieces):
        for way in range(2):
            arrive(way, i)
        if i + AHEAD < 2 * pieces:
            send_own(i + AHEAD)
        if i > AHEAD and far_done < pieces:
            for way in range(2):
                arrive_far(way, far_done)
            far_done += 1
        if i == 0:
            bytes_of(n1.at[pl.ds(0, PLANE - 1)], n1_recv)
            bytes_of(n1.at[pl.ds(0, PLANE - 1)], n_send)
            nz[zero] = jnp.sum(n1[...], axis=0)
            for j in (4, 5, 3, 6, 2, 7, 1):
                remote(nz.at[zero], nz.at[zero], n_send, nz_recv, at_zero(zero + j)).start()
        if i == 5:
            bytes_of(nz.at[pl.ds(0, ZERO - 1)], nz_recv)
            bytes_of(nz.at[pl.ds(0, ZERO - 1)], n_send)

            @pl.when(high >= 2)
            def _():
                to = {"zero": zero, "model": other_plane}
                remote(nz, n3, n_send, n3_recv, to).start()

        if i == 10:

            @pl.when(high >= 2)
            def _():
                bytes_of(n3, n3_recv)
                bytes_of(n3, n_send)
                to = lax.rem(zero + 2 * (2 * high - 5) + ZERO, ZERO)
                remote(n3, n3, n_send, n3_recv, at_zero(to)).start()

    @pl.when(high >= 2)
    def _():
        bytes_of(n3, n_send)

    @pl.when(high < 2)
    def _():
        bytes_of(n3, n3_recv)

    for z in range(ZERO):
        wide[z * 5 : z * 5 + 5, :] = (nz[z] + n3[z])[0:5]
    norm[...] = wide[...].astype(bf16)

    for way in range(2):
        bytes_of(rg.at[:, pl.ds(0, 3 * wide_n)], send_sem.at[way])
    bytes_of(rg, d2d_send)
    for a in range(2):
        bytes_of(rg.at[:, pl.ds(0, 4 * wide_n)], d2d_recv.at[a])


def local(w_gate, first_gate, second_gate, w_up, first_up, second_up, norm_train, norm_step):
    weights = [v.T for v in (w_gate, first_gate, second_gate, w_up, first_up, second_up)]
    n, d = weights[0].shape
    small = norm_train.shape[0]
    pieces = n // CHUNK
    vmem, hbm = pl.BlockSpec(memory_space=pltpu.VMEM), pl.BlockSpec(memory_space=pltpu.HBM)
    dma = pltpu.SemaphoreType.DMA
    rg, ru, lg, lu, cols, norm = pl.pallas_call(
        kernel,
        out_shape=(
            pltpu.VMEM((n, ZERO * d), bf16),
            pltpu.VMEM((n, ZERO * d), bf16),
            pltpu.VMEM((n, d), f32),
            pltpu.VMEM((n, d), f32),
            pltpu.VMEM((8, LANES), f32),
            pltpu.VMEM((ZERO * MODEL * small // LANES, LANES), bf16),
        ),
        in_specs=[hbm] * 8,
        out_specs=(vmem,) * 6,
        scratch_shapes=[
            pltpu.VMEM((6, n, d), f32),
            pltpu.VMEM((2, small), f32),
            pltpu.VMEM((ZERO, 8, LANES), f32),
            pltpu.VMEM((PLANE, 8, LANES), f32),
            pltpu.VMEM((ZERO, 8, LANES), f32),
            pltpu.VMEM((ZERO, 8, LANES), f32),
            pltpu.VMEM((ZERO * MODEL * small // LANES, LANES), f32),
            dma((6, pieces)),
            dma((2,)),
            dma(()),
            dma(()),
            dma(()),
            dma(()),
            dma(()),
            dma(()),
            dma((2,)),
            dma((2, 2 * pieces)),
            dma((2, pieces)),
            dma(()),
            dma((2,)),
        ],
        compiler_params=pltpu.CompilerParams(
            collective_id=0, has_side_effects=True, vmem_limit_bytes=48 * 1024 * 1024
        ),
        name="update_gather",
    )(*weights, norm_train.reshape(1, small), norm_step.reshape(1, small))
    flat = cols.reshape(2, 4 * LANES)
    return rg.T, ru.T, flat[0, :n], flat[1, :n], norm.reshape(-1), lg.T, lu.T


def solution(mesh):
    return jax.shard_map(
        local,
        mesh=mesh,
        in_specs=(P("zero", "model"),) * 6 + (P(("zero", "model")),) * 2,
        out_specs=(
            P(None, "model"),
            P(None, "model"),
            P("model"),
            P("model"),
            P(),
            P("zero", "model"),
            P("zero", "model"),
        ),
        check_vma=False,
    )
```

```python
import functools

import jax
import jax.numpy as jnp
from jax import lax
from jax.experimental import pallas as pl
from jax.experimental.pallas import tpu as pltpu
from jax.sharding import PartitionSpec as P

learn_rate = 0.25
hold_rate = 0.8

LANES = 128
CHUNK = 48
AHEAD = 4
WRITES = 4
ZERO, MODEL, PLANE = 8, 32, 16

f32, bf16 = jnp.float32, jnp.bfloat16


def iota(shape, dim):
    return lax.broadcasted_iota(jnp.int32, shape, dim)


def kernel(
    wg, fg, sg, wu, fu, su, nt, ns,
    rg, ru, lg, lu, cg, cu, norm,
    stage, raw, nin, mx, n1, nz, n3, wide,
    in_sem, nin_sem, mx_send, mx_recv, n_send, n1_recv, nz_recv, n3_recv,
    send_sem, own_recv, fwd_recv, d2d_send, d2d_recv,
):
    zero, model = lax.axis_index("zero"), lax.axis_index("model")
    rows_n, wide_n = lg.shape
    pieces = rows_n // CHUNK
    gathered, latest = (rg, ru), (lg, lu)
    high = lax.div(zero, 2)

    def at_zero(z):
        return {"zero": lax.rem(z, ZERO), "model": model}

    right, left = lax.rem(zero + 2, ZERO), lax.rem(zero + 6, ZERO)
    far = lax.rem(zero + 4, ZERO)
    mate = zero + 1 - 2 * lax.rem(zero, 2)
    plane0 = lax.div(model, PLANE) * PLANE
    spot = model - plane0
    other_plane = lax.rem(model + PLANE, MODEL)

    barrier = pltpu.get_barrier_semaphore()
    for j in range(1, ZERO):
        pl.semaphore_signal(barrier, inc=1, device_id=at_zero(zero + j))
    for j in range(1, PLANE):
        pl.semaphore_signal(
            barrier, inc=1, device_id={"zero": zero, "model": plane0 + lax.rem(spot + j, PLANE)}
        )

    @pl.when(high >= 2)
    def _():
        pl.semaphore_signal(barrier, inc=1, device_id={"zero": zero, "model": other_plane})

    loads = {}
    for k in range(pieces):
        for a, group in enumerate(((wg, fg, sg), (wu, fu, su))):
            for i, ref in enumerate(group):
                rows = pl.ds(k * CHUNK, CHUNK)
                loads[a, k, i] = pltpu.make_async_copy(
                    ref.at[rows], stage.at[a * 3 + i, rows], in_sem.at[a * 3 + i, k]
                )
                loads[a, k, i].start()
    norm_loads = [
        pltpu.make_async_copy(ref, nin.at[pl.ds(i, 1)], nin_sem.at[i])
        for i, ref in enumerate((nt, ns))
    ]
    for c in norm_loads:
        c.start()

    best = [None] * 8
    for k in range(pieces):
        rows = slice(k * CHUNK, (k + 1) * CHUNK)
        for a in range(2):
            for i in range(3):
                loads[a, k, i].wait()
            w, first, second = (stage[a * 3 + i, rows, :] for i in range(3))
            hold = hold_rate * first + second
            new = w - learn_rate * hold
            latest[a][rows, :] = new
            top = jnp.max(jnp.abs(new), axis=1, keepdims=True)
            at = iota((CHUNK, LANES), 0) + k * CHUNK - iota((CHUNK, LANES), 1)
            for r in range(k * CHUNK // LANES, ((k + 1) * CHUNK - 1) // LANES + 1):
                line = jnp.max(jnp.where(at == r * LANES, top, 0.0), axis=0, keepdims=True)
                old = best[a * 4 + r]
                best[a * 4 + r] = line if old is None else jnp.maximum(old, line)
    for r in range(8):
        mx[zero, pl.ds(r, 1), :] = best[r]

    for c in norm_loads:
        c.wait()
    part = jnp.concatenate(
        [nin[0:1, :] + nin[1:2, :], jnp.zeros((1, LANES - nin.shape[1]), f32)], axis=1
    ).astype(bf16).astype(f32)
    width = nin.shape[1]
    begin = model * width
    lane0 = lax.rem(begin, LANES)
    turned = pltpu.roll(jnp.broadcast_to(part, (8, LANES)), lane0, 1)
    place = iota((8, LANES), 0) * LANES + iota((8, LANES), 1) - begin
    n1[spot] = jnp.where((place >= 0) & (place < width), turned, 0.0)

    @pl.when(high < 2)
    def _():
        pl.semaphore_wait(barrier, ZERO - 1 + PLANE - 1)

    @pl.when(high >= 2)
    def _():
        pl.semaphore_wait(barrier, ZERO - 1 + PLANE)

    def remote(src, dst, send, recv, to):
        return pltpu.make_async_remote_copy(
            src_ref=src, dst_ref=dst, send_sem=send, recv_sem=recv, device_id=to,
            device_id_type=pl.DeviceIdType.MESH,
        )

    def bytes_of(ref, sem):
        pltpu.make_async_copy(ref, ref, sem).wait()

    for j in (4, 5, 3, 6, 2, 7, 1):
        remote(mx.at[zero], mx.at[zero], mx_send, mx_recv, at_zero(zero + j)).start()
    for way, to in enumerate((right, left)):
        remote(
            latest[way].at[pl.ds(0, CHUNK)], raw.at[way], send_sem.at[way], own_recv.at[way, 0], at_zero(to)
        ).start()
    for j in range(1, PLANE):
        to = {"zero": zero, "model": plane0 + lax.rem(spot + j, PLANE)}
        remote(n1.at[spot], n1.at[spot], n_send, n1_recv, to).start()

    bytes_of(mx.at[pl.ds(0, ZERO - 1)], mx_recv)
    bytes_of(mx.at[pl.ds(0, ZERO - 1)], mx_send)
    most = jnp.max(mx[...], axis=0)
    for r in range(4):
        some = min(LANES, rows_n - r * LANES)
        cg[:, r * LANES : r * LANES + some] = most[r : r + 1, :some]
        cu[:, r * LANES : r * LANES + some] = most[4 + r : 5 + r, :some]

    def part_of(a, k, z):
        return gathered[a].at[pl.ds(k * CHUNK, CHUNK), pl.ds(pl.multiple_of(z * wide_n, LANES), wide_n)]

    def rate_of(a, k):
        at = iota((CHUNK, LANES), 0) + k * CHUNK - iota((CHUNK, LANES), 1)
        top = None
        for r in range(k * CHUNK // LANES, ((k + 1) * CHUNK - 1) // LANES + 1):
            line = jnp.broadcast_to(most[a * 4 + r : a * 4 + r + 1], (CHUNK, LANES))
            part = jnp.max(jnp.where(at == r * LANES, line, 0.0), axis=1, keepdims=True)
            top = part if top is None else jnp.maximum(top, part)
        return 1.0 / top

    def keep(a, k, z, values, rate):
        columns = pl.ds(pl.multiple_of(z * wide_n, LANES), wide_n)
        gathered[a][k * CHUNK : (k + 1) * CHUNK, columns] = (values * rate).astype(bf16)

    rates0 = [rate_of(a, 0) for a in range(2)]

    def normalise(k):
        for a in range(2):
            rate = rates0[a] if k == 0 else rate_of(a, k)
            keep(a, k, zero, latest[a][k * CHUNK : (k + 1) * CHUNK, :], rate)

    def push(a, k, z):
        ref = part_of(a, k, z)
        remote(ref, ref, d2d_send, d2d_recv.at[a], at_zero(mate)).start()

    steps = [(0, k) for k in range(pieces)] + [(1, k) for k in range(pieces)]

    def send_own(i):
        a, k = steps[i]
        if i < pieces:
            normalise(k)
        for way, (b, to) in enumerate(((a, right), (1 - a, left))):
            if i == 0:
                continue
            ref = part_of(b, k, zero)
            remote(ref, ref, send_sem.at[way], own_recv.at[way, i], at_zero(to)).start()
        if i < pieces:
            push(0, k, zero)
            push(1, k, zero)

    def arrive(way, i):
        a, k = steps[i]
        b, origin = ((a, left), (1 - a, right))[way]
        ref = part_of(b, k, origin)
        if i == 0:
            bytes_of(raw.at[way], own_recv.at[way, 0])
            keep(b, k, origin, raw[way], rates0[b])
        else:
            remote(ref, ref, send_sem.at[way], own_recv.at[way, i], at_zero(origin)).wait_recv()
        if i < pieces:
            to = (right, left)[way]
            remote(ref, ref, send_sem.at[way], fwd_recv.at[way, k], at_zero(to)).start()
        push(b, k, origin)

    def arrive_far(way, k):
        ref = part_of(way, k, far)
        remote(ref, ref, send_sem.at[way], fwd_recv.at[way, k], at_zero(far)).wait_recv()
        push(way, k, far)

    for i in range(AHEAD):
        send_own(i)
    far_done = 0
    for i in range(2 * pieces):
        for way in range(2):
            arrive(way, i)
        if i + AHEAD < 2 * pieces:
            send_own(i + AHEAD)
        if i > AHEAD and far_done < pieces:
            for way in range(2):
                arrive_far(way, far_done)
            far_done += 1
        if i == 0:
            bytes_of(n1.at[pl.ds(0, PLANE - 1)], n1_recv)
            bytes_of(n1.at[pl.ds(0, PLANE - 1)], n_send)
            nz[zero] = jnp.sum(n1[...], axis=0)
            for j in (4, 5, 3, 6, 2, 7, 1):
                remote(nz.at[zero], nz.at[zero], n_send, nz_recv, at_zero(zero + j)).start()
        if i == 5:
            bytes_of(nz.at[pl.ds(0, ZERO - 1)], nz_recv)
            bytes_of(nz.at[pl.ds(0, ZERO - 1)], n_send)

            @pl.when(high >= 2)
            def _():
                to = {"zero": zero, "model": other_plane}
                remote(nz, n3, n_send, n3_recv, to).start()

        if i == 10:

            @pl.when(high >= 2)
            def _():
                bytes_of(n3, n3_recv)
                bytes_of(n3, n_send)
                to = lax.rem(zero + 2 * (2 * high - 5) + ZERO, ZERO)
                remote(n3, n3, n_send, n3_recv, at_zero(to)).start()

    @pl.when(high >= 2)
    def _():
        bytes_of(n3, n_send)

    @pl.when(high < 2)
    def _():
        bytes_of(n3, n3_recv)

    for z in range(ZERO):
        wide[z * 5 : z * 5 + 5, :] = (nz[z] + n3[z])[0:5]
    norm[...] = wide[...].astype(bf16)

    for way in range(2):
        bytes_of(rg.at[pl.ds(0, (rows_n * 3 + CHUNK) // 4), pl.ds(0, 4 * wide_n)], send_sem.at[way])
    bytes_of(rg, d2d_send)
    for a in range(2):
        bytes_of(rg.at[:, pl.ds(0, 4 * wide_n)], d2d_recv.at[a])


def writer(rg, ru, lg, lu, cg, cu, norm, rg_o, ru_o, cg_o, cu_o, norm_o, lg_o, lu_o, sems):
    copies = []

    def out(src, dst):
        copies.append(pltpu.make_async_copy(src, dst, sems.at[len(copies)]))
        copies[-1].start()

    n = rg.shape[0]
    step = -(-n // WRITES // 8) * 8
    for src, dst in ((rg, rg_o), (ru, ru_o)):
        for at in range(0, n, step):
            rows = pl.ds(at, min(step, n - at))
            out(src.at[rows], dst.at[rows])
    out(lg, lg_o)
    out(lu, lu_o)
    out(cg, cg_o)
    out(cu, cu_o)
    out(norm, norm_o)
    for c in copies:
        c.wait()


def local(w_gate, first_gate, second_gate, w_up, first_up, second_up, norm_train, norm_step):
    weights = [v.T for v in (w_gate, first_gate, second_gate, w_up, first_up, second_up)]
    n, d = weights[0].shape
    small = norm_train.shape[0]
    pieces = n // CHUNK
    lines = ZERO * MODEL * small // LANES
    vmem, hbm = pl.BlockSpec(memory_space=pltpu.VMEM), pl.BlockSpec(memory_space=pltpu.HBM)
    dma = pltpu.SemaphoreType.DMA
    held = pl.pallas_call(
        kernel,
        out_shape=(
            pltpu.VMEM((n, ZERO * d), bf16),
            pltpu.VMEM((n, ZERO * d), bf16),
            pltpu.VMEM((n, d), f32),
            pltpu.VMEM((n, d), f32),
            pltpu.VMEM((1, n), f32),
            pltpu.VMEM((1, n), f32),
            pltpu.VMEM((lines, LANES), bf16),
        ),
        in_specs=[hbm] * 8,
        out_specs=(vmem,) * 7,
        scratch_shapes=[
            pltpu.VMEM((6, n, d), f32),
            pltpu.VMEM((2, CHUNK, d), f32),
            pltpu.VMEM((2, small), f32),
            pltpu.VMEM((ZERO, 8, LANES), f32),
            pltpu.VMEM((PLANE, 8, LANES), f32),
            pltpu.VMEM((ZERO, 8, LANES), f32),
            pltpu.VMEM((ZERO, 8, LANES), f32),
            pltpu.VMEM((lines, LANES), f32),
            dma((6, pieces)),
            dma((2,)),
            dma(()),
            dma(()),
            dma(()),
            dma(()),
            dma(()),
            dma(()),
            dma((2,)),
            dma((2, 2 * pieces)),
            dma((2, pieces)),
            dma(()),
            dma((2,)),
        ],
        compiler_params=pltpu.CompilerParams(
            collective_id=0, has_side_effects=True, vmem_limit_bytes=48 * 1024 * 1024
        ),
        name="update_gather",
    )(*weights, norm_train.reshape(1, small), norm_step.reshape(1, small))
    rg, ru, cg, cu, norm, lg, lu = pl.pallas_call(
        writer,
        out_shape=(
            pltpu.HBM((n, ZERO * d), bf16),
            pltpu.HBM((n, ZERO * d), bf16),
            pltpu.HBM((1, n), f32),
            pltpu.HBM((1, n), f32),
            pltpu.HBM((lines, LANES), bf16),
            pltpu.HBM((n, d), f32),
            pltpu.HBM((n, d), f32),
        ),
        in_specs=[vmem] * 7,
        out_specs=(hbm,) * 7,
        scratch_shapes=[dma((2 * WRITES + 5,))],
        compiler_params=pltpu.CompilerParams(vmem_limit_bytes=48 * 1024 * 1024),
        name="write_out",
    )(*[pltpu.with_memory_space_constraint(v, pltpu.VMEM) for v in held])
    return rg.T, ru.T, cg.reshape(-1), cu.reshape(-1), norm.reshape(-1), lg.T, lu.T


def solution(mesh):
    return jax.shard_map(
        local,
        mesh=mesh,
        in_specs=(P("zero", "model"),) * 6 + (P(("zero", "model")),) * 2,
        out_specs=(
            P(None, "model"),
            P(None, "model"),
            P("model"),
            P("model"),
            P(),
            P("zero", "model"),
            P("zero", "model"),
        ),
        check_vma=False,
    )
```

```python
import functools

import jax
import jax.numpy as jnp
from jax import lax
from jax.experimental import pallas as pl
from jax.experimental.pallas import tpu as pltpu
from jax.sharding import PartitionSpec as P

learn_rate = 0.25
hold_rate = 0.8

LANES = 128
CHUNK = 48
AHEAD = 4
EARLY = 1
LOADS = 3
WRITES = 4
ZERO, MODEL, SIDE = 8, 32, 4

f32, bf16 = jnp.float32, jnp.bfloat16


def iota(shape, dim):
    return lax.broadcasted_iota(jnp.int32, shape, dim)


def kernel(
    wg, fg, sg, wu, fu, su, nt, ns,
    rg, ru, lg, lu, cg, cu, norm,
    stage, raw, peak, nin, mx, n1, n2, nz, n3, wide,
    in_sem, nin_sem, mx_send, mx_recv, n_send, n1_recv, n2_recv, nz_recv, n3_recv,
    send_sem, own_recv, fwd_recv, d2d_send, d2d_recv,
):
    zero, model = lax.axis_index("zero"), lax.axis_index("model")
    rows_n, wide_n = lg.shape
    pieces = rows_n // CHUNK
    gathered, latest = (rg, ru), (lg, lu)
    high = lax.div(zero, 2)

    def at_zero(z):
        return {"zero": lax.rem(z, ZERO), "model": model}

    right, left = lax.rem(zero + 2, ZERO), lax.rem(zero + 6, ZERO)
    far = lax.rem(zero + 4, ZERO)
    mate = zero + 1 - 2 * lax.rem(zero, 2)
    x, y = lax.rem(model, SIDE), lax.rem(lax.div(model, SIDE), SIDE)
    other_plane = lax.rem(model + MODEL // 2, MODEL)

    def at_x(j):
        return {"zero": zero, "model": model - x + lax.rem(x + j, SIDE)}

    def at_y(j):
        return {"zero": zero, "model": model + (lax.rem(y + j, SIDE) - y) * SIDE}

    barrier = pltpu.get_barrier_semaphore()
    for j in range(1, ZERO):
        pl.semaphore_signal(barrier, inc=1, device_id=at_zero(zero + j))
    for j in range(1, SIDE):
        pl.semaphore_signal(barrier, inc=1, device_id=at_x(j))
        pl.semaphore_signal(barrier, inc=1, device_id=at_y(j))

    @pl.when(high >= 2)
    def _():
        pl.semaphore_signal(barrier, inc=1, device_id={"zero": zero, "model": other_plane})

    loads = {}
    some = rows_n // LOADS
    for k in range(LOADS):
        for a, group in enumerate(((wg, fg, sg), (wu, fu, su))):
            for i, ref in enumerate(group):
                rows = pl.ds(k * some, some)
                loads[a, k, i] = pltpu.make_async_copy(
                    ref.at[rows], stage.at[a * 3 + i, rows], in_sem.at[a * 3 + i, k]
                )
                loads[a, k, i].start()
    norm_loads = [
        pltpu.make_async_copy(ref, nin.at[pl.ds(i, 1)], nin_sem.at[i])
        for i, ref in enumerate((nt, ns))
    ]
    for c in norm_loads:
        c.start()

    for k in range(pieces):
        rows = slice(k * CHUNK, (k + 1) * CHUNK)
        for a in range(2):
            if k * CHUNK % some == 0:
                for i in range(3):
                    loads[a, k * CHUNK // some, i].wait()
            w, first, second = (stage[a * 3 + i, rows, :] for i in range(3))
            hold = hold_rate * first + second
            new = w - learn_rate * hold
            latest[a][rows, :] = new
            size = jnp.abs(new)
            tall = size[:, :LANES]
            for at in range(LANES, wide_n, LANES):
                tall = jnp.maximum(tall, size[:, at : at + LANES])
            peak[a, rows, :] = tall
    best = [None] * 8
    for k in range(pieces):
        for a in range(2):
            top = jnp.max(peak[a, k * CHUNK : (k + 1) * CHUNK, :], axis=1, keepdims=True)
            at = iota((CHUNK, LANES), 0) + k * CHUNK - iota((CHUNK, LANES), 1)
            for r in range(k * CHUNK // LANES, ((k + 1) * CHUNK - 1) // LANES + 1):
                line = jnp.max(jnp.where(at == r * LANES, top, 0.0), axis=0, keepdims=True)
                old = best[a * 4 + r]
                best[a * 4 + r] = line if old is None else jnp.maximum(old, line)
    for r in range(8):
        mx[zero, pl.ds(r, 1), :] = best[r]

    for c in norm_loads:
        c.wait()
    part = jnp.concatenate(
        [nin[0:1, :] + nin[1:2, :], jnp.zeros((1, LANES - nin.shape[1]), f32)], axis=1
    ).astype(bf16).astype(f32)
    width = nin.shape[1]
    begin = model * width
    lane0 = lax.rem(begin, LANES)
    turned = pltpu.roll(jnp.broadcast_to(part, (8, LANES)), lane0, 1)
    place = iota((8, LANES), 0) * LANES + iota((8, LANES), 1) - begin
    n1[x] = jnp.where((place >= 0) & (place < width), turned, 0.0)

    @pl.when(high < 2)
    def _():
        pl.semaphore_wait(barrier, ZERO - 1 + 2 * (SIDE - 1))

    @pl.when(high >= 2)
    def _():
        pl.semaphore_wait(barrier, ZERO + 2 * (SIDE - 1))

    def remote(src, dst, send, recv, to):
        return pltpu.make_async_remote_copy(
            src_ref=src, dst_ref=dst, send_sem=send, recv_sem=recv, device_id=to,
            device_id_type=pl.DeviceIdType.MESH,
        )

    def bytes_of(ref, sem):
        pltpu.make_async_copy(ref, ref, sem).wait()

    for j in (4, 5, 3, 6, 2, 7, 1):
        remote(mx.at[zero], mx.at[zero], mx_send, mx_recv, at_zero(zero + j)).start()
    for i in range(EARLY):
        for way, to in enumerate((right, left)):
            remote(
                latest[way].at[pl.ds(i * CHUNK, CHUNK)],
                raw.at[way, i],
                send_sem.at[way],
                own_recv.at[way, i],
                at_zero(to),
            ).start()
    for j in range(1, SIDE):
        remote(n1.at[x], n1.at[x], n_send, n1_recv, at_x(j)).start()

    bytes_of(mx.at[pl.ds(0, ZERO - 1)], mx_recv)
    bytes_of(mx.at[pl.ds(0, ZERO - 1)], mx_send)
    most = jnp.max(mx[...], axis=0)
    for r in range(4):
        some = min(LANES, rows_n - r * LANES)
        cg[:, r * LANES : r * LANES + some] = most[r : r + 1, :some]
        cu[:, r * LANES : r * LANES + some] = most[4 + r : 5 + r, :some]

    def part_of(a, k, z):
        return gathered[a].at[pl.ds(k * CHUNK, CHUNK), pl.ds(pl.multiple_of(z * wide_n, LANES), wide_n)]

    def rate_of(a, k):
        at = iota((CHUNK, LANES), 0) + k * CHUNK - iota((CHUNK, LANES), 1)
        top = None
        for r in range(k * CHUNK // LANES, ((k + 1) * CHUNK - 1) // LANES + 1):
            line = jnp.broadcast_to(most[a * 4 + r : a * 4 + r + 1], (CHUNK, LANES))
            part = jnp.max(jnp.where(at == r * LANES, line, 0.0), axis=1, keepdims=True)
            top = part if top is None else jnp.maximum(top, part)
        return 1.0 / top

    def keep(a, k, z, values, rate):
        columns = pl.ds(pl.multiple_of(z * wide_n, LANES), wide_n)
        gathered[a][k * CHUNK : (k + 1) * CHUNK, columns] = (values * rate).astype(bf16)

    rates = {}

    def normalise(k):
        for a in range(2):
            rates[a, k] = rate_of(a, k)
            keep(a, k, zero, latest[a][k * CHUNK : (k + 1) * CHUNK, :], rates[a, k])

    def push(a, k, z):
        ref = part_of(a, k, z)
        remote(ref, ref, d2d_send, d2d_recv.at[a], at_zero(mate)).start()

    gain_at = [2 * pieces * v // 18 for v in (0, 2, 6, 11, 15)]
    steps = [(0, k) for k in range(pieces)] + [(1, k) for k in range(pieces)]

    def send_own(i):
        a, k = steps[i]
        if i < pieces:
            normalise(k)
        for way, (b, to) in enumerate(((a, right), (1 - a, left))):
            if i < EARLY:
                continue
            ref = part_of(b, k, zero)
            remote(ref, ref, send_sem.at[way], own_recv.at[way, i], at_zero(to)).start()
        if i < pieces:
            push(0, k, zero)
            push(1, k, zero)

    def arrive(way, i):
        a, k = steps[i]
        b, origin = ((a, left), (1 - a, right))[way]
        ref = part_of(b, k, origin)
        if i < EARLY:
            bytes_of(raw.at[way, i], own_recv.at[way, i])
            keep(b, k, origin, raw[way, i], rates[b, k])
        else:
            remote(ref, ref, send_sem.at[way], own_recv.at[way, i], at_zero(origin)).wait_recv()
        if i < pieces:
            to = (right, left)[way]
            remote(ref, ref, send_sem.at[way], fwd_recv.at[way, k], at_zero(to)).start()
        push(b, k, origin)

    def arrive_far(way, k):
        ref = part_of(way, k, far)
        remote(ref, ref, send_sem.at[way], fwd_recv.at[way, k], at_zero(far)).wait_recv()
        push(way, k, far)

    for i in range(AHEAD):
        send_own(i)
    far_done = 0
    for i in range(2 * pieces):
        for way in range(2):
            arrive(way, i)
        if i + AHEAD < 2 * pieces:
            send_own(i + AHEAD)
        if i > AHEAD and far_done < pieces:
            for way in range(2):
                arrive_far(way, far_done)
            far_done += 1
        if i == gain_at[0]:
            bytes_of(n1.at[pl.ds(0, SIDE - 1)], n1_recv)
            bytes_of(n1.at[pl.ds(0, SIDE - 1)], n_send)
            n2[y] = jnp.sum(n1[...], axis=0)
            for j in range(1, SIDE):
                remote(n2.at[y], n2.at[y], n_send, n2_recv, at_y(j)).start()
        if i == gain_at[1]:
            bytes_of(n2.at[pl.ds(0, SIDE - 1)], n2_recv)
            bytes_of(n2.at[pl.ds(0, SIDE - 1)], n_send)
            nz[zero] = jnp.sum(n2[...], axis=0)
            for j in (4, 5, 3, 6, 2, 7, 1):
                remote(nz.at[zero], nz.at[zero], n_send, nz_recv, at_zero(zero + j)).start()
        if i == gain_at[2]:
            bytes_of(nz.at[pl.ds(0, ZERO - 1)], nz_recv)
            bytes_of(nz.at[pl.ds(0, ZERO - 1)], n_send)

            @pl.when(high >= 2)
            def _():
                to = {"zero": zero, "model": other_plane}
                remote(nz, n3, n_send, n3_recv, to).start()

        if i == gain_at[3]:

            @pl.when(high >= 2)
            def _():
                bytes_of(n3, n3_recv)
                bytes_of(n3, n_send)
                to = lax.rem(zero + 2 * (2 * high - 5) + ZERO, ZERO)
                remote(n3, n3, n_send, n3_recv, at_zero(to)).start()

        if i == gain_at[4]:
            @pl.when(high >= 2)
            def _():
                bytes_of(n3, n_send)

            @pl.when(high < 2)
            def _():
                bytes_of(n3, n3_recv)

            for z in range(ZERO):
                wide[z * 5 : z * 5 + 5, :] = (nz[z] + n3[z])[0:5]
            norm[...] = wide[...].astype(bf16)

    for way in range(2):
        total = rows_n * 3 + EARLY * CHUNK
        blocks = next(b for b in range(3, ZERO + 1) if total % (8 * b) == 0 and total // b <= rows_n)
        bytes_of(rg.at[pl.ds(0, total // blocks), pl.ds(0, blocks * wide_n)], send_sem.at[way])
    bytes_of(rg, d2d_send)
    for a in range(2):
        bytes_of(rg.at[:, pl.ds(0, 4 * wide_n)], d2d_recv.at[a])


def writer(rg, ru, lg, lu, cg, cu, norm, rg_o, ru_o, cg_o, cu_o, norm_o, lg_o, lu_o, sems):
    copies = []

    def out(src, dst):
        copies.append(pltpu.make_async_copy(src, dst, sems.at[len(copies)]))
        copies[-1].start()

    n = rg.shape[0]
    step = -(-n // WRITES // 8) * 8
    for src, dst in ((rg, rg_o), (ru, ru_o)):
        for at in range(0, n, step):
            rows = pl.ds(at, min(step, n - at))
            out(src.at[rows], dst.at[rows])
    out(lg, lg_o)
    out(lu, lu_o)
    out(cg, cg_o)
    out(cu, cu_o)
    out(norm, norm_o)
    for c in copies:
        c.wait()


def local(w_gate, first_gate, second_gate, w_up, first_up, second_up, norm_train, norm_step):
    weights = [v.T for v in (w_gate, first_gate, second_gate, w_up, first_up, second_up)]
    n, d = weights[0].shape
    small = norm_train.shape[0]
    pieces = n // CHUNK
    lines = ZERO * MODEL * small // LANES
    vmem, hbm = pl.BlockSpec(memory_space=pltpu.VMEM), pl.BlockSpec(memory_space=pltpu.HBM)
    dma = pltpu.SemaphoreType.DMA
    held = pl.pallas_call(
        kernel,
        out_shape=(
            pltpu.VMEM((n, ZERO * d), bf16),
            pltpu.VMEM((n, ZERO * d), bf16),
            pltpu.VMEM((n, d), f32),
            pltpu.VMEM((n, d), f32),
            pltpu.VMEM((1, n), f32),
            pltpu.VMEM((1, n), f32),
            pltpu.VMEM((lines, LANES), bf16),
        ),
        in_specs=[hbm] * 8,
        out_specs=(vmem,) * 7,
        scratch_shapes=[
            pltpu.VMEM((6, n, d), f32),
            pltpu.VMEM((2, max(EARLY, 1), CHUNK, d), f32),
            pltpu.VMEM((2, n, LANES), f32),
            pltpu.VMEM((2, small), f32),
            pltpu.VMEM((ZERO, 8, LANES), f32),
            pltpu.VMEM((SIDE, 8, LANES), f32),
            pltpu.VMEM((SIDE, 8, LANES), f32),
            pltpu.VMEM((ZERO, 8, LANES), f32),
            pltpu.VMEM((ZERO, 8, LANES), f32),
            pltpu.VMEM((lines, LANES), f32),
            dma((6, LOADS)),
            dma((2,)),
            dma(()),
            dma(()),
            dma(()),
            dma(()),
            dma(()),
            dma(()),
            dma(()),
            dma((2,)),
            dma((2, 2 * pieces)),
            dma((2, pieces)),
            dma(()),
            dma((2,)),
        ],
        compiler_params=pltpu.CompilerParams(
            collective_id=0, has_side_effects=True, vmem_limit_bytes=48 * 1024 * 1024
        ),
        name="update_gather",
    )(*weights, norm_train.reshape(1, small), norm_step.reshape(1, small))
    rg, ru, cg, cu, norm, lg, lu = pl.pallas_call(
        writer,
        out_shape=(
            pltpu.HBM((n, ZERO * d), bf16),
            pltpu.HBM((n, ZERO * d), bf16),
            pltpu.HBM((1, n), f32),
            pltpu.HBM((1, n), f32),
            pltpu.HBM((lines, LANES), bf16),
            pltpu.HBM((n, d), f32),
            pltpu.HBM((n, d), f32),
        ),
        in_specs=[vmem] * 7,
        out_specs=(hbm,) * 7,
        scratch_shapes=[dma((2 * WRITES + 5,))],
        compiler_params=pltpu.CompilerParams(vmem_limit_bytes=48 * 1024 * 1024),
        name="write_out",
    )(*[pltpu.with_memory_space_constraint(v, pltpu.VMEM) for v in held])
    return rg.T, ru.T, cg.reshape(-1), cu.reshape(-1), norm.reshape(-1), lg.T, lu.T


def solution(mesh):
    return jax.shard_map(
        local,
        mesh=mesh,
        in_specs=(P("zero", "model"),) * 6 + (P(("zero", "model")),) * 2,
        out_specs=(
            P(None, "model"),
            P(None, "model"),
            P("model"),
            P("model"),
            P(),
            P("zero", "model"),
            P("zero", "model"),
        ),
        check_vma=False,
    )
```

```python
import functools

import jax
import jax.numpy as jnp
from jax import lax
from jax.experimental import pallas as pl
from jax.experimental.pallas import tpu as pltpu
from jax.sharding import PartitionSpec as P

learn_rate = 0.25
hold_rate = 0.8

LANES = 128
CHUNK = 48
AHEAD = 6
EARLY = 1
LOADS = 3
WRITES = 4
ZERO, MODEL, SIDE = 8, 32, 4

f32, bf16 = jnp.float32, jnp.bfloat16


def iota(shape, dim):
    return lax.broadcasted_iota(jnp.int32, shape, dim)


def kernel(
    wg, fg, sg, wu, fu, su, nt, ns,
    rg, ru, lg, lu, cg, cu, norm,
    stage, raw, peak, nin, mx, n1, n2, n3, nz, wide,
    in_sem, nin_sem, mx_send, mx_recv, n_send, n1_recv, n2_recv, n3_recv, nz_recv, nm_recv,
    early_send, send_sem, own_recv, fwd_recv, d2d_send, d2d_recv,
):
    zero, model = lax.axis_index("zero"), lax.axis_index("model")
    rows_n, wide_n = lg.shape
    pieces = rows_n // CHUNK
    gathered, latest = (rg, ru), (lg, lu)

    def at_zero(z):
        return {"zero": lax.rem(z, ZERO), "model": model}

    right, left = lax.rem(zero + 2, ZERO), lax.rem(zero + 6, ZERO)
    far = lax.rem(zero + 4, ZERO)
    mate = zero + 1 - 2 * lax.rem(zero, 2)
    x, y = lax.rem(model, SIDE), lax.rem(lax.div(model, SIDE), SIDE)
    beside = {"zero": zero, "model": lax.rem(model + MODEL // 2, MODEL)}

    def at_x(j):
        return {"zero": zero, "model": model - x + lax.rem(x + j, SIDE)}

    def at_y(j):
        return {"zero": zero, "model": model + (lax.rem(y + j, SIDE) - y) * SIDE}

    barrier = pltpu.get_barrier_semaphore()
    for j in range(1, ZERO):
        pl.semaphore_signal(barrier, inc=1, device_id=at_zero(zero + j))
    for j in range(1, SIDE):
        pl.semaphore_signal(barrier, inc=1, device_id=at_x(j))
        pl.semaphore_signal(barrier, inc=1, device_id=at_y(j))

    pl.semaphore_signal(barrier, inc=1, device_id=beside)

    loads = {}
    some = rows_n // LOADS
    for k in range(LOADS):
        for a, group in enumerate(((wg, fg, sg), (wu, fu, su))):
            for i, ref in enumerate(group):
                rows = pl.ds(k * some, some)
                loads[a, k, i] = pltpu.make_async_copy(
                    ref.at[rows], stage.at[a * 3 + i, rows], in_sem.at[a * 3 + i, k]
                )
                loads[a, k, i].start()
    norm_loads = [
        pltpu.make_async_copy(ref, nin.at[pl.ds(i, 1)], nin_sem.at[i])
        for i, ref in enumerate((nt, ns))
    ]
    for c in norm_loads:
        c.start()

    for k in range(pieces):
        rows = slice(k * CHUNK, (k + 1) * CHUNK)
        for a in range(2):
            if k * CHUNK % some == 0:
                for i in range(3):
                    loads[a, k * CHUNK // some, i].wait()
            w, first, second = (stage[a * 3 + i, rows, :] for i in range(3))
            hold = hold_rate * first + second
            new = w - learn_rate * hold
            latest[a][rows, :] = new
            size = jnp.abs(new)
            tall = size[:, :LANES]
            for at in range(LANES, wide_n, LANES):
                tall = jnp.maximum(tall, size[:, at : at + LANES])
            peak[a, rows, :] = tall
    best = [None] * 8
    for k in range(pieces):
        for a in range(2):
            top = jnp.max(peak[a, k * CHUNK : (k + 1) * CHUNK, :], axis=1, keepdims=True)
            at = iota((CHUNK, LANES), 0) + k * CHUNK - iota((CHUNK, LANES), 1)
            for r in range(k * CHUNK // LANES, ((k + 1) * CHUNK - 1) // LANES + 1):
                line = jnp.max(jnp.where(at == r * LANES, top, 0.0), axis=0, keepdims=True)
                old = best[a * 4 + r]
                best[a * 4 + r] = line if old is None else jnp.maximum(old, line)
    for r in range(8):
        mx[zero, pl.ds(r, 1), :] = best[r]

    for c in norm_loads:
        c.wait()
    part = jnp.concatenate(
        [nin[0:1, :] + nin[1:2, :], jnp.zeros((1, LANES - nin.shape[1]), f32)], axis=1
    ).astype(bf16).astype(f32)
    width = nin.shape[1]
    begin = model * width
    lane0 = lax.rem(begin, LANES)
    turned = pltpu.roll(jnp.broadcast_to(part, (8, LANES)), lane0, 1)
    place = iota((8, LANES), 0) * LANES + iota((8, LANES), 1) - begin
    n1[x] = jnp.where((place >= 0) & (place < width), turned, 0.0).astype(bf16)

    pl.semaphore_wait(barrier, ZERO + 2 * (SIDE - 1))

    def remote(src, dst, send, recv, to):
        return pltpu.make_async_remote_copy(
            src_ref=src, dst_ref=dst, send_sem=send, recv_sem=recv, device_id=to,
            device_id_type=pl.DeviceIdType.MESH,
        )

    def bytes_of(ref, sem):
        pltpu.make_async_copy(ref, ref, sem).wait()

    for j in (4, 5, 3, 6, 2, 7, 1):
        remote(mx.at[zero], mx.at[zero], mx_send, mx_recv, at_zero(zero + j)).start()
    for i in range(EARLY):
        for way, to in enumerate((right, left)):
            remote(
                latest[way].at[pl.ds(i * CHUNK, CHUNK)],
                raw.at[way, i],
                early_send,
                own_recv.at[way, i],
                at_zero(to),
            ).start()
    for j in range(1, SIDE):
        remote(n1.at[x], n1.at[x], n_send, n1_recv, at_x(j)).start()

    bytes_of(mx.at[pl.ds(0, ZERO - 1)], mx_recv)
    bytes_of(mx.at[pl.ds(0, ZERO - 1)], mx_send)
    most = jnp.max(mx[...], axis=0)
    for r in range(4):
        some = min(LANES, rows_n - r * LANES)
        cg[:, r * LANES : r * LANES + some] = most[r : r + 1, :some]
        cu[:, r * LANES : r * LANES + some] = most[4 + r : 5 + r, :some]

    def part_of(a, k, z):
        return gathered[a].at[pl.ds(k * CHUNK, CHUNK), pl.ds(pl.multiple_of(z * wide_n, LANES), wide_n)]

    def rate_of(a, k):
        at = iota((CHUNK, LANES), 0) + k * CHUNK - iota((CHUNK, LANES), 1)
        top = None
        for r in range(k * CHUNK // LANES, ((k + 1) * CHUNK - 1) // LANES + 1):
            line = jnp.broadcast_to(most[a * 4 + r : a * 4 + r + 1], (CHUNK, LANES))
            part = jnp.max(jnp.where(at == r * LANES, line, 0.0), axis=1, keepdims=True)
            top = part if top is None else jnp.maximum(top, part)
        return 1.0 / top

    def keep(a, k, z, values, rate):
        columns = pl.ds(pl.multiple_of(z * wide_n, LANES), wide_n)
        gathered[a][k * CHUNK : (k + 1) * CHUNK, columns] = (values * rate).astype(bf16)

    rates = {}

    def normalise(k):
        for a in range(2):
            rates[a, k] = rate_of(a, k)
            keep(a, k, zero, latest[a][k * CHUNK : (k + 1) * CHUNK, :], rates[a, k])

    def push(a, k, z):
        ref = part_of(a, k, z)
        remote(ref, ref, d2d_send, d2d_recv.at[a], at_zero(mate)).start()

    gain_at = [2 * pieces * v // 18 for v in (0, 2, 5, 9, 14)]
    steps = [(0, k) for k in range(pieces)] + [(1, k) for k in range(pieces)]

    def send_own(i):
        a, k = steps[i]
        if i < pieces:
            normalise(k)
        for way, (b, to) in enumerate(((a, right), (1 - a, left))):
            if i < EARLY:
                continue
            ref = part_of(b, k, zero)
            remote(ref, ref, send_sem.at[way], own_recv.at[way, i], at_zero(to)).start()
        if i < pieces:
            push(0, k, zero)
            push(1, k, zero)

    def arrive(way, i):
        a, k = steps[i]
        b, origin = ((a, left), (1 - a, right))[way]
        ref = part_of(b, k, origin)
        if i < EARLY:
            bytes_of(raw.at[way, i], own_recv.at[way, i])
            keep(b, k, origin, raw[way, i], rates[b, k])
        else:
            remote(ref, ref, send_sem.at[way], own_recv.at[way, i], at_zero(origin)).wait_recv()
        if i < pieces:
            to = (right, left)[way]
            remote(ref, ref, send_sem.at[way], fwd_recv.at[way, k], at_zero(to)).start()
        push(b, k, origin)

    def arrive_far(way, k):
        ref = part_of(way, k, far)
        remote(ref, ref, send_sem.at[way], fwd_recv.at[way, k], at_zero(far)).wait_recv()
        push(way, k, far)

    for i in range(AHEAD):
        send_own(i)
    far_done = 0
    for i in range(2 * pieces):
        for way in range(2):
            arrive(way, i)
        if i + AHEAD < 2 * pieces:
            send_own(i + AHEAD)
        if i > AHEAD and far_done < pieces:
            for way in range(2):
                arrive_far(way, far_done)
            far_done += 1
        if i == gain_at[0]:
            bytes_of(n1.at[pl.ds(0, SIDE - 1)], n1_recv)
            bytes_of(n1.at[pl.ds(0, SIDE - 1)], n_send)
            n2[y] = jnp.sum(n1[...].astype(f32), axis=0).astype(bf16)
            for j in range(1, SIDE):
                remote(n2.at[y], n2.at[y], n_send, n2_recv, at_y(j)).start()
        if i == gain_at[1]:
            bytes_of(n2.at[pl.ds(0, SIDE - 1)], n2_recv)
            bytes_of(n2.at[pl.ds(0, SIDE - 1)], n_send)
            n3[0] = jnp.sum(n2[...].astype(f32), axis=0).astype(bf16)
            remote(n3.at[0], n3.at[1], n_send, n3_recv, beside).start()
        if i == gain_at[2]:
            bytes_of(n3.at[1], n3_recv)
            bytes_of(n3.at[0], n_send)
            nz[zero] = jnp.sum(n3[...].astype(f32), axis=0).astype(bf16)
            for z in (far, left, right):
                remote(nz.at[zero], nz.at[zero], n_send, nz_recv, at_zero(z)).start()
        if i == gain_at[3]:
            bytes_of(nz.at[pl.ds(0, 3)], nz_recv)
            bytes_of(nz.at[pl.ds(0, 3)], n_send)
            for z in (zero, far, left, right):
                remote(nz.at[z], nz.at[z], n_send, nm_recv, at_zero(mate)).start()
        if i == gain_at[4]:
            bytes_of(nz.at[pl.ds(0, 4)], nm_recv)
            bytes_of(nz.at[pl.ds(0, 4)], n_send)
            for z in range(ZERO):
                wide[z * 5 : z * 5 + 5, :] = nz[z].astype(f32)[0:5]
            norm[...] = wide[...].astype(bf16)

    for way in range(2):
        total = rows_n * 3 - EARLY * CHUNK
        blocks = next(b for b in range(3, ZERO + 1) if total % (8 * b) == 0 and total // b <= rows_n)
        bytes_of(rg.at[pl.ds(0, total // blocks), pl.ds(0, blocks * wide_n)], send_sem.at[way])
    if EARLY:
        bytes_of(raw, early_send)
    bytes_of(rg, d2d_send)
    for a in range(2):
        bytes_of(rg.at[:, pl.ds(0, 4 * wide_n)], d2d_recv.at[a])


def writer(rg, ru, lg, lu, cg, cu, norm, rg_o, ru_o, cg_o, cu_o, norm_o, lg_o, lu_o, sems):
    copies = []

    def out(src, dst):
        copies.append(pltpu.make_async_copy(src, dst, sems.at[len(copies)]))
        copies[-1].start()

    n = rg.shape[0]
    step = -(-n // WRITES // 8) * 8
    for src, dst in ((rg, rg_o), (ru, ru_o)):
        for at in range(0, n, step):
            rows = pl.ds(at, min(step, n - at))
            out(src.at[rows], dst.at[rows])
    out(lg, lg_o)
    out(lu, lu_o)
    out(cg, cg_o)
    out(cu, cu_o)
    out(norm, norm_o)
    for c in copies:
        c.wait()


def local(w_gate, first_gate, second_gate, w_up, first_up, second_up, norm_train, norm_step):
    weights = [v.T for v in (w_gate, first_gate, second_gate, w_up, first_up, second_up)]
    n, d = weights[0].shape
    small = norm_train.shape[0]
    pieces = n // CHUNK
    lines = ZERO * MODEL * small // LANES
    vmem, hbm = pl.BlockSpec(memory_space=pltpu.VMEM), pl.BlockSpec(memory_space=pltpu.HBM)
    dma = pltpu.SemaphoreType.DMA
    held = pl.pallas_call(
        kernel,
        out_shape=(
            pltpu.VMEM((n, ZERO * d), bf16),
            pltpu.VMEM((n, ZERO * d), bf16),
            pltpu.VMEM((n, d), f32),
            pltpu.VMEM((n, d), f32),
            pltpu.VMEM((1, n), f32),
            pltpu.VMEM((1, n), f32),
            pltpu.VMEM((lines, LANES), bf16),
        ),
        in_specs=[hbm] * 8,
        out_specs=(vmem,) * 7,
        scratch_shapes=[
            pltpu.VMEM((6, n, d), f32),
            pltpu.VMEM((2, max(EARLY, 1), CHUNK, d), f32),
            pltpu.VMEM((2, n, LANES), f32),
            pltpu.VMEM((2, small), f32),
            pltpu.VMEM((ZERO, 8, LANES), f32),
            pltpu.VMEM((SIDE, 8, LANES), bf16),
            pltpu.VMEM((SIDE, 8, LANES), bf16),
            pltpu.VMEM((2, 8, LANES), bf16),
            pltpu.VMEM((ZERO, 8, LANES), bf16),
            pltpu.VMEM((lines, LANES), f32),
            dma((6, LOADS)),
            dma((2,)),
            dma(()),
            dma(()),
            dma(()),
            dma(()),
            dma(()),
            dma(()),
            dma(()),
            dma(()),
            dma(()),
            dma((2,)),
            dma((2, 2 * pieces)),
            dma((2, pieces)),
            dma(()),
            dma((2,)),
        ],
        compiler_params=pltpu.CompilerParams(
            collective_id=0, has_side_effects=True, vmem_limit_bytes=48 * 1024 * 1024
        ),
        name="update_gather",
    )(*weights, norm_train.reshape(1, small), norm_step.reshape(1, small))
    rg, ru, cg, cu, norm, lg, lu = pl.pallas_call(
        writer,
        out_shape=(
            pltpu.HBM((n, ZERO * d), bf16),
            pltpu.HBM((n, ZERO * d), bf16),
            pltpu.HBM((1, n), f32),
            pltpu.HBM((1, n), f32),
            pltpu.HBM((lines, LANES), bf16),
            pltpu.HBM((n, d), f32),
            pltpu.HBM((n, d), f32),
        ),
        in_specs=[vmem] * 7,
        out_specs=(hbm,) * 7,
        scratch_shapes=[dma((2 * WRITES + 5,))],
        compiler_params=pltpu.CompilerParams(vmem_limit_bytes=48 * 1024 * 1024),
        name="write_out",
    )(*[pltpu.with_memory_space_constraint(v, pltpu.VMEM) for v in held])
    return rg.T, ru.T, cg.reshape(-1), cu.reshape(-1), norm.reshape(-1), lg.T, lu.T


def solution(mesh):
    return jax.shard_map(
        local,
        mesh=mesh,
        in_specs=(P("zero", "model"),) * 6 + (P(("zero", "model")),) * 2,
        out_specs=(
            P(None, "model"),
            P(None, "model"),
            P("model"),
            P("model"),
            P(),
            P("zero", "model"),
            P("zero", "model"),
        ),
        check_vma=False,
    )
```

```python
import functools

import jax
import jax.numpy as jnp
from jax import lax
from jax.experimental import pallas as pl
from jax.experimental.pallas import tpu as pltpu
from jax.sharding import PartitionSpec as P

learn_rate = 0.25
hold_rate = 0.8

LANES = 128
CHUNK = 48
AHEAD = 6
SOONER = 6
LOADS = 3
WRITES = 4
ZERO, MODEL, SIDE = 8, 32, 4

f32, bf16 = jnp.float32, jnp.bfloat16


def iota(shape, dim):
    return lax.broadcasted_iota(jnp.int32, shape, dim)


def other_core(z):
    return z + 1 - 2 * lax.rem(z, 2)


def at_zero(z):
    return {"zero": lax.rem(z, ZERO), "model": lax.axis_index("model")}


def remote(src, dst, send, recv, to):
    return pltpu.make_async_remote_copy(
        src_ref=src, dst_ref=dst, send_sem=send, recv_sem=recv, device_id=to,
        device_id_type=pl.DeviceIdType.MESH,
    )


def bytes_of(ref, sem):
    pltpu.make_async_copy(ref, ref, sem).wait()


def lines_of(k):
    at = iota((CHUNK, LANES), 0) + k * CHUNK - iota((CHUNK, LANES), 1)
    return [(r, at == r * LANES) for r in range(k * CHUNK // LANES, ((k + 1) * CHUNK - 1) // LANES + 1)]


def goes_right(a, k):
    return (a + k) % 2 == 0


def exchange(items, gathered, latest, most, wide_n, sems, raw=None, early_send=None, beside_step=None):
    send_sem, fwd_send, own_recv, fwd_recv, d2d_send, d2d_recv = sems
    zero = lax.axis_index("zero")
    right, left = lax.rem(zero + 2, ZERO), lax.rem(zero + 6, ZERO)
    far, mate = lax.rem(zero + 4, ZERO), other_core(zero)
    groups = [it for it in items if goes_right(*it)], [it for it in items if not goes_right(*it)]
    orders = groups[0] + groups[1], groups[1] + groups[0]
    early = 0 if raw is None else 1
    n = len(items)

    def part_of(item, z):
        a, k = item
        columns = pl.ds(pl.multiple_of(z * wide_n, LANES), wide_n)
        return gathered[a].at[pl.ds(k * CHUNK, CHUNK), columns]

    def rows_wait(rows, sem):
        ref = next(g for g in gathered if g is not None)
        blocks = next(b for b in range(1, ZERO + 1) if rows % (8 * b) == 0 and rows // b <= ref.shape[0])
        bytes_of(ref.at[pl.ds(0, rows // blocks), pl.ds(0, blocks * wide_n)], sem)

    rates = {}

    def rate_of(item):
        if item not in rates:
            a, k = item
            top = None
            for r, mine in lines_of(k):
                line = jnp.broadcast_to(most[a * 4 + r : a * 4 + r + 1], (CHUNK, LANES))
                part = jnp.max(jnp.where(mine, line, 0.0), axis=1, keepdims=True)
                top = part if top is None else jnp.maximum(top, part)
            rates[item] = 1.0 / top
        return rates[item]

    def keep(item, z, values):
        a, k = item
        columns = pl.ds(pl.multiple_of(z * wide_n, LANES), wide_n)
        gathered[a][k * CHUNK : (k + 1) * CHUNK, columns] = (values * rate_of(item)).astype(bf16)

    def push(item, z):
        ref = part_of(item, z)
        remote(ref, ref, d2d_send, d2d_recv, at_zero(mate)).start()

    ready = set()

    def send_own(i):
        fresh = [it for it in dict.fromkeys((orders[0][i], orders[1][i])) if it not in ready]
        for a, k in fresh:
            keep((a, k), zero, latest[a][k * CHUNK : (k + 1) * CHUNK, :])
            ready.add((a, k))
        if i >= early:
            for way, to in enumerate((right, left)):
                ref = part_of(orders[way][i], zero)
                remote(ref, ref, send_sem.at[way], own_recv.at[way, i], at_zero(to)).start()
        for item in fresh:
            push(item, zero)

    def arrive(way, i):
        item, origin = orders[way][i], (left, right)[way]
        ref = part_of(item, origin)
        if i < early:
            bytes_of(raw.at[way], own_recv.at[way, i])
            keep(item, origin, raw[way])
        else:
            remote(ref, ref, send_sem.at[way], own_recv.at[way, i], at_zero(origin)).wait_recv()
        if i < len(groups[way]):
            to = (right, left)[way]
            remote(ref, ref, fwd_send.at[way], fwd_recv.at[way, i], at_zero(to)).start()
        push(item, origin)

    def arrive_far(i):
        for way in range(2):
            if i < len(groups[way]):
                ref = part_of(groups[way][i], far)
                remote(ref, ref, fwd_send.at[way], fwd_recv.at[way, i], at_zero(far)).wait_recv()
                push(groups[way][i], far)

    most_far = max(len(g) for g in groups)
    for i in range(min(AHEAD, n)):
        send_own(i)
    far_done = 0
    for i in range(n):
        for way in range(2):
            arrive(way, i)
        if i + AHEAD < n:
            send_own(i + AHEAD)
        if i > AHEAD and far_done < most_far:
            arrive_far(far_done)
            far_done += 1
        if beside_step is not None:
            beside_step(i, n)
    for i in range(far_done, most_far):
        arrive_far(i)

    for way in range(2):
        rows_wait((n - early) * CHUNK, send_sem.at[way])
        if groups[way]:
            rows_wait(len(groups[way]) * CHUNK, fwd_send.at[way])
    if early:
        bytes_of(raw, early_send)
    rows_wait(4 * n * CHUNK, d2d_send)
    rows_wait(4 * n * CHUNK, d2d_recv)


def kernel(
    wg, fg, sg, wu, fu, su, nt, ns,
    rg, ru, lg, lu, cg, cu, norm, most_ref,
    stage, raw, peak, nin, mx, n1, n2, n3, nz, wide,
    in_sem, nin_sem, mx_send, mx_recv, n_send, n1_recv, n2_recv, n3_recv, nz_recv, nm_recv,
    early_send, *sems,
):
    zero, model = lax.axis_index("zero"), lax.axis_index("model")
    rows_n, wide_n = lg.shape
    pieces = rows_n // CHUNK
    gathered, latest = (rg, ru), (lg, lu)

    right, left = lax.rem(zero + 2, ZERO), lax.rem(zero + 6, ZERO)
    far = lax.rem(zero + 4, ZERO)
    mate = zero + 1 - 2 * lax.rem(zero, 2)
    x, y = lax.rem(model, SIDE), lax.rem(lax.div(model, SIDE), SIDE)
    beside = {"zero": zero, "model": lax.rem(model + MODEL // 2, MODEL)}

    def at_x(j):
        return {"zero": zero, "model": model - x + lax.rem(x + j, SIDE)}

    def at_y(j):
        return {"zero": zero, "model": model + (lax.rem(y + j, SIDE) - y) * SIDE}

    barrier = pltpu.get_barrier_semaphore()
    for j in range(1, ZERO):
        pl.semaphore_signal(barrier, inc=1, device_id=at_zero(zero + j))
    for j in range(1, SIDE):
        pl.semaphore_signal(barrier, inc=1, device_id=at_x(j))
        pl.semaphore_signal(barrier, inc=1, device_id=at_y(j))

    pl.semaphore_signal(barrier, inc=1, device_id=beside)

    loads = {}
    some = rows_n // LOADS
    for k in range(LOADS):
        for a, group in enumerate(((wg, fg, sg), (wu, fu, su))):
            for i, ref in enumerate(group):
                rows = pl.ds(k * some, some)
                loads[a, k, i] = pltpu.make_async_copy(
                    ref.at[rows], stage.at[a * 3 + i, rows], in_sem.at[a * 3 + i, k]
                )
                loads[a, k, i].start()
    norm_loads = [
        pltpu.make_async_copy(ref, nin.at[pl.ds(i, 1)], nin_sem.at[i])
        for i, ref in enumerate((nt, ns))
    ]
    for c in norm_loads:
        c.start()

    for k in range(pieces):
        rows = slice(k * CHUNK, (k + 1) * CHUNK)
        for a in range(2):
            if k * CHUNK % some == 0:
                for i in range(3):
                    loads[a, k * CHUNK // some, i].wait()
            w, first, second = (stage[a * 3 + i, rows, :] for i in range(3))
            hold = hold_rate * first + second
            new = w - learn_rate * hold
            latest[a][rows, :] = new
            size = jnp.abs(new)
            tall = size[:, :LANES]
            for at in range(LANES, wide_n, LANES):
                tall = jnp.maximum(tall, size[:, at : at + LANES])
            peak[a, rows, :] = tall
    best = [None] * 8
    for k in range(pieces):
        for a in range(2):
            top = jnp.max(peak[a, k * CHUNK : (k + 1) * CHUNK, :], axis=1, keepdims=True)
            at = iota((CHUNK, LANES), 0) + k * CHUNK - iota((CHUNK, LANES), 1)
            for r in range(k * CHUNK // LANES, ((k + 1) * CHUNK - 1) // LANES + 1):
                line = jnp.max(jnp.where(at == r * LANES, top, 0.0), axis=0, keepdims=True)
                old = best[a * 4 + r]
                best[a * 4 + r] = line if old is None else jnp.maximum(old, line)
    for r in range(8):
        mx[zero, pl.ds(r, 1), :] = best[r]

    for c in norm_loads:
        c.wait()
    part = jnp.concatenate(
        [nin[0:1, :] + nin[1:2, :], jnp.zeros((1, LANES - nin.shape[1]), f32)], axis=1
    ).astype(bf16).astype(f32)
    width = nin.shape[1]
    begin = model * width
    lane0 = lax.rem(begin, LANES)
    turned = pltpu.roll(jnp.broadcast_to(part, (8, LANES)), lane0, 1)
    place = iota((8, LANES), 0) * LANES + iota((8, LANES), 1) - begin
    n1[x] = jnp.where((place >= 0) & (place < width), turned, 0.0).astype(bf16)

    pl.semaphore_wait(barrier, ZERO + 2 * (SIDE - 1))

    for j in (4, 5, 3, 6, 2, 7, 1):
        remote(mx.at[zero], mx.at[zero], mx_send, mx_recv, at_zero(zero + j)).start()
    for way, to in enumerate((right, left)):
        rows = pl.ds(way * CHUNK, CHUNK)
        remote(lg.at[rows], raw.at[way], early_send, sems[2].at[way, 0], at_zero(to)).start()
    for j in range(1, SIDE):
        remote(n1.at[x], n1.at[x], n_send, n1_recv, at_x(j)).start()

    bytes_of(mx.at[pl.ds(0, ZERO - 1)], mx_recv)
    bytes_of(mx.at[pl.ds(0, ZERO - 1)], mx_send)
    most = jnp.max(mx[...], axis=0)
    most_ref[...] = most
    for r in range(4):
        some = min(LANES, rows_n - r * LANES)
        cg[:, r * LANES : r * LANES + some] = most[r : r + 1, :some]
        cu[:, r * LANES : r * LANES + some] = most[4 + r : 5 + r, :some]

    def gain_step(i, n):
        marks = [n * v // 18 for v in (0, 2, 5, 9, 14)]
        if i == marks[0]:
            bytes_of(n1.at[pl.ds(0, SIDE - 1)], n1_recv)
            bytes_of(n1.at[pl.ds(0, SIDE - 1)], n_send)
            n2[y] = jnp.sum(n1[...].astype(f32), axis=0).astype(bf16)
            for j in range(1, SIDE):
                remote(n2.at[y], n2.at[y], n_send, n2_recv, at_y(j)).start()
        if i == marks[1]:
            bytes_of(n2.at[pl.ds(0, SIDE - 1)], n2_recv)
            bytes_of(n2.at[pl.ds(0, SIDE - 1)], n_send)
            n3[0] = jnp.sum(n2[...].astype(f32), axis=0).astype(bf16)
            remote(n3.at[0], n3.at[1], n_send, n3_recv, beside).start()
        if i == marks[2]:
            bytes_of(n3.at[1], n3_recv)
            bytes_of(n3.at[0], n_send)
            nz[zero] = jnp.sum(n3[...].astype(f32), axis=0).astype(bf16)
            for z in (far, left, right):
                remote(nz.at[zero], nz.at[zero], n_send, nz_recv, at_zero(z)).start()
        if i == marks[3]:
            bytes_of(nz.at[pl.ds(0, 3)], nz_recv)
            bytes_of(nz.at[pl.ds(0, 3)], n_send)
            for z in (zero, far, left, right):
                remote(nz.at[z], nz.at[z], n_send, nm_recv, at_zero(mate)).start()
        if i == marks[4]:
            bytes_of(nz.at[pl.ds(0, 4)], nm_recv)
            bytes_of(nz.at[pl.ds(0, 4)], n_send)
            for z in range(ZERO):
                wide[z * 5 : z * 5 + 5, :] = nz[z].astype(f32)[0:5]
            norm[...] = wide[...].astype(bf16)

    gates = [(0, k) for k in range(pieces)]
    for odd, items in enumerate((gates, gates + [(1, k) for k in range(SOONER)])):

        @pl.when(lax.div(model, MODEL // 2) == odd)
        def _():
            exchange(items, gathered, latest, most, wide_n, sems, raw, early_send, gain_step)


def later_kernel(lu, most_ref, ru, *sems):
    zero, model = lax.axis_index("zero"), lax.axis_index("model")
    rows_n, wide_n = lu.shape
    barrier = pltpu.get_barrier_semaphore()
    for z in (zero + 2, zero + 6, other_core(zero)):
        pl.semaphore_signal(barrier, inc=1, device_id=at_zero(z))
    pl.semaphore_wait(barrier, 3)
    most = most_ref[...]
    ups = [(1, k) for k in range(rows_n // CHUNK)]
    for odd, items in enumerate((ups, ups[SOONER:])):

        @pl.when(lax.div(model, MODEL // 2) == odd)
        def _():
            exchange(items, (None, ru), (None, lu), most, wide_n, sems)


def write(pairs, sems):
    copies = []
    for src, dst, parts in pairs:
        n = src.shape[0]
        step = n if parts == 1 else -(-n // parts // 8) * 8
        for at in range(0, n, step):
            rows = pl.ds(at, min(step, n - at))
            whole = parts == 1
            copies.append(
                pltpu.make_async_copy(
                    src if whole else src.at[rows], dst if whole else dst.at[rows], sems.at[len(copies)]
                )
            )
            copies[-1].start()
    for c in copies:
        c.wait()


def writer(rg, lg, lu, cg, cu, norm, rg_o, cg_o, cu_o, norm_o, lg_o, lu_o, sems):
    write(
        [(rg, rg_o, WRITES), (lg, lg_o, 1), (lu, lu_o, 1), (cg, cg_o, 1), (cu, cu_o, 1), (norm, norm_o, 1)],
        sems,
    )


def later_writer(sooner, later, ru_o, sems):
    n = later.shape[0]
    cut = SOONER * CHUNK
    for odd in range(2):

        @pl.when(lax.div(lax.axis_index("model"), MODEL // 2) == odd)
        def _():
            if odd:
                pairs = [(sooner.at[pl.ds(0, cut)], ru_o.at[pl.ds(0, cut)], WRITES)]
                pairs.append((later.at[pl.ds(cut, n - cut)], ru_o.at[pl.ds(cut, n - cut)], 2))
            else:
                pairs = [(later, ru_o, WRITES)]
            write(pairs, sems)


def local(w_gate, first_gate, second_gate, w_up, first_up, second_up, norm_train, norm_step):
    weights = [v.T for v in (w_gate, first_gate, second_gate, w_up, first_up, second_up)]
    n, d = weights[0].shape
    small = norm_train.shape[0]
    pieces = n // CHUNK
    lines = ZERO * MODEL * small // LANES
    vmem, hbm = pl.BlockSpec(memory_space=pltpu.VMEM), pl.BlockSpec(memory_space=pltpu.HBM)
    dma = pltpu.SemaphoreType.DMA
    limit, low = 48 * 1024 * 1024, 8 * 1024 * 1024

    def in_vmem(*values):
        return [pltpu.with_memory_space_constraint(v, pltpu.VMEM) for v in values]

    def sems_for(count):
        return [dma((2,)), dma((2,)), dma((2, count)), dma((2, count)), dma(()), dma(())]

    rg, sooner, lg, lu, cg, cu, norm, most = pl.pallas_call(
        kernel,
        out_shape=(
            pltpu.VMEM((n, ZERO * d), bf16),
            pltpu.VMEM((n, ZERO * d), bf16),
            pltpu.VMEM((n, d), f32),
            pltpu.VMEM((n, d), f32),
            pltpu.VMEM((1, n), f32),
            pltpu.VMEM((1, n), f32),
            pltpu.VMEM((lines, LANES), bf16),
            pltpu.VMEM((8, LANES), f32),
        ),
        in_specs=[hbm] * 8,
        out_specs=(vmem,) * 8,
        scratch_shapes=[
            pltpu.VMEM((6, n, d), f32),
            pltpu.VMEM((2, CHUNK, d), f32),
            pltpu.VMEM((2, n, LANES), f32),
            pltpu.VMEM((2, small), f32),
            pltpu.VMEM((ZERO, 8, LANES), f32),
            pltpu.VMEM((SIDE, 8, LANES), bf16),
            pltpu.VMEM((SIDE, 8, LANES), bf16),
            pltpu.VMEM((2, 8, LANES), bf16),
            pltpu.VMEM((ZERO, 8, LANES), bf16),
            pltpu.VMEM((lines, LANES), f32),
            dma((6, LOADS)),
            dma((2,)),
            *[dma(())] * 9,
            *sems_for(pieces + SOONER),
        ],
        compiler_params=pltpu.CompilerParams(
            collective_id=0, has_side_effects=True, vmem_limit_bytes=limit
        ),
        name="update_gather",
    )(*weights, norm_train.reshape(1, small), norm_step.reshape(1, small))
    rg, cg, cu, norm, lg_o, lu_o = pl.pallas_call(
        writer,
        out_shape=(
            pltpu.HBM((n, ZERO * d), bf16),
            pltpu.HBM((1, n), f32),
            pltpu.HBM((1, n), f32),
            pltpu.HBM((lines, LANES), bf16),
            pltpu.HBM((n, d), f32),
            pltpu.HBM((n, d), f32),
        ),
        in_specs=[vmem] * 6,
        out_specs=(hbm,) * 6,
        scratch_shapes=[dma((WRITES + 5,))],
        compiler_params=pltpu.CompilerParams(has_side_effects=True, vmem_limit_bytes=low),
        name="write_out",
    )(*in_vmem(rg, lg, lu, cg, cu, norm))
    most, rg = lax.optimization_barrier((most, rg))
    later = pl.pallas_call(
        later_kernel,
        out_shape=pltpu.VMEM((n, ZERO * d), bf16),
        in_specs=[vmem] * 2,
        out_specs=vmem,
        scratch_shapes=sems_for(pieces),
        compiler_params=pltpu.CompilerParams(
            collective_id=1, has_side_effects=True, vmem_limit_bytes=low
        ),
        name="later_gather",
    )(*in_vmem(lu, most))
    ru = pl.pallas_call(
        later_writer,
        out_shape=pltpu.HBM((n, ZERO * d), bf16),
        in_specs=[vmem] * 2,
        out_specs=hbm,
        scratch_shapes=[dma((WRITES + 2,))],
        compiler_params=pltpu.CompilerParams(vmem_limit_bytes=low),
        name="write_later",
    )(*in_vmem(sooner, later))
    return rg.T, ru.T, cg.reshape(-1), cu.reshape(-1), norm.reshape(-1), lg_o.T, lu_o.T


def solution(mesh):
    return jax.shard_map(
        local,
        mesh=mesh,
        in_specs=(P("zero", "model"),) * 6 + (P(("zero", "model")),) * 2,
        out_specs=(
            P(None, "model"),
            P(None, "model"),
            P("model"),
            P("model"),
            P(),
            P("zero", "model"),
            P("zero", "model"),
        ),
        check_vma=False,
    )
```
